32 devices in a mesh: scan: 8 (over y, x, core), grp: 4 (over z).
Axes of the slice: x: 2, y: 2, z: 4, core: 2. Of those that a mesh axis runs over, the one named last changes fastest.
Arguments:
- frames: bfloat16 [256, 1024, 1024], P('scan', 'grp'), may hold values from -6 to 6
- dark_frame: int32 [36864], replicated, may hold values from 0 to 15
- gain_frame: int32 [36864], replicated, may hold values from 3072 to 5120
- bf_index: int32 [1024], replicated, may hold values from 0 to 36863
- row_level: float32 [256], P('scan'), may hold values from 0.5 to 2
- shift_num: int32 [2, 1024], P(None, ('scan', 'grp')), may hold values from -32 to 32
Outputs:
- upsampled: float32 [512, 2048], P(('scan', 'grp'))
- correlation: float32 [1024, 256], P(('scan', 'grp'))
The draws below stay inside these ranges and needn't reach their ends.
All inputs are finite; a program needn't handle non-finite values.
Results may differ from the reference program's by a relative error of at most 0.0085.
Values may be sent and summed in bfloat16 or wider, within the bound.
A program may use at most 128 MiB of HBM per device.

```python
import math
import jax
import jax.numpy as jnp
from jax import lax

SY = 256
SX = 1024
BF = 1024
DET = 36864
LAGS = 16
DEN = 4


def set_ends(entries, own_key, least, top_value):
    shape = entries.shape
    spot = [jax.random.randint(jax.random.fold_in(own_key, axis), (), 0, shape[axis]) for axis in range(len(shape))]
    entries = entries.at[tuple(spot)].set(least)
    longest = shape.index(max(shape))
    spot[longest] = (spot[longest] + 1) % shape[longest]
    return entries.at[tuple(spot)].set(top_value)


def steps_of(rng, extent, split, low, top_value):
    loudness, own = 1.0, jax.random.fold_in(rng, 6)
    for position, blocks in split:
        draws = jnp.exp(jax.random.uniform(jax.random.fold_in(own, position), (blocks,), jnp.float32, low / len(split), top_value / len(split)))
        loudness = loudness * jnp.repeat(draws, extent[position] // blocks).reshape([-1 if axis == position else 1 for axis in range(len(extent))])
    return loudness


def bell_draw(own_key, extent, deviation, reach, pieces=(), kind=jnp.bfloat16):
    array = jax.random.normal(own_key, extent, jnp.float32) * deviation
    if len(pieces) > 0:
        array = steps_of(own_key, extent, pieces, -0.22, 0.18) * array
    return jnp.clip(array, min=-reach, max=reach).astype(kind)


def setup_inputs(seed: int = 0) -> dict:
    key_list = jax.random.split(jax.random.key(seed), 7)
    return {
        "frames": bell_draw(key_list[0], (SY, SX, BF), 1.0, 6.0, ((0, 8), (1, 4))),
        "dark_frame": set_ends(jax.random.randint(key_list[1], (DET,), 0, 16), jax.random.fold_in(key_list[1], 1), 0, 15).astype(jnp.int32),
        "gain_frame": set_ends(jax.random.randint(key_list[2], (DET,), 3072, 5121), jax.random.fold_in(key_list[2], 1), 3072, 5120).astype(jnp.int32),
        "bf_index": set_ends(jax.random.randint(key_list[3], (BF,), 0, DET), jax.random.fold_in(key_list[3], 1), 0, DET - 1).astype(jnp.int32),
        "row_level": jnp.clip(jnp.exp(math.log(2.0) - 1.3862944 * jax.random.uniform(key_list[4], (SY,), jnp.float32) ** steps_of(key_list[4], (SY,), ((0, 8),), -0.2, 0.2)), 0.5, 2.0),
        "shift_num": set_ends(jax.random.randint(key_list[5], (2, BF), -32, 33), jax.random.fold_in(key_list[5], 1), -32, 32).astype(jnp.int32),
    }


def signed_freq(length):
    indices = jnp.arange(length, dtype=jnp.int32)
    return jnp.where(indices < length // 2, indices, indices - length)

def phase_pair(leading, trailing, period):
    product = jnp.mod(leading[:, None] * trailing[None, :], period)
    angles = product.astype(jnp.float32) * (2.0 * math.pi / period)
    return (jnp.cos(angles), jnp.sin(angles))

def matmul(left, right):
    return jnp.dot(left.astype(jnp.float32), right.astype(jnp.float32), precision=lax.Precision.HIGHEST, preferred_element_type=jnp.float32)

def forward_pair(picture, cosine_cols, sine_cols, cosine_rows, sine_rows):
    real_rows = matmul(picture, cosine_cols).astype(jnp.bfloat16)
    imag_rows = (-matmul(picture, sine_cols)).astype(jnp.bfloat16)
    real_part = matmul(cosine_rows, real_rows) + matmul(sine_rows, imag_rows)
    imag_part = matmul(cosine_rows, imag_rows) - matmul(sine_rows, real_rows)
    anchor = (jnp.arange(real_part.shape[0])[:, None] == 0) & (jnp.arange(real_part.shape[1])[None, :] == 0)
    return (jnp.where(anchor, 0.0, real_part), jnp.where(anchor, 0.0, imag_part))

def axis_phase(length, amount):
    product = jnp.mod(signed_freq(length) * amount, DEN * length)
    angles = product.astype(jnp.float32) * (2.0 * math.pi / (DEN * length))
    return (jnp.cos(angles), jnp.sin(angles))

def shift_apply(real_part, imag_part, amounts):
    cosine_y, sine_y = axis_phase(real_part.shape[0], amounts[0])
    cosine_x, sine_x = axis_phase(real_part.shape[1], amounts[1])
    cos_phi = cosine_y[:, None] * cosine_x[None, :] - sine_y[:, None] * sine_x[None, :]
    sin_phi = sine_y[:, None] * cosine_x[None, :] + cosine_y[:, None] * sine_x[None, :]
    real_shift = (real_part * cos_phi + imag_part * sin_phi).astype(jnp.bfloat16)
    imag_shift = (imag_part * cos_phi - real_part * sin_phi).astype(jnp.bfloat16)
    return (real_shift, imag_shift)

def correlate(real_part, imag_part, ref_real, ref_imag, lag_tables, scale):
    lag_rows_cos, lag_rows_sin, lag_cols_cos, lag_cols_sin = lag_tables
    cross_real = (real_part * ref_real + imag_part * ref_imag).astype(jnp.bfloat16)
    cross_imag = (imag_part * ref_real - real_part * ref_imag).astype(jnp.bfloat16)
    half_real = matmul(lag_rows_cos, cross_real) - matmul(lag_rows_sin, cross_imag)
    half_imag = matmul(lag_rows_cos, cross_imag) + matmul(lag_rows_sin, cross_real)
    return ((matmul(half_real, lag_cols_cos) - matmul(half_imag, lag_cols_sin)) * scale).reshape(-1)

def reference(frames, dark_frame, gain_frame, bf_index, row_level, shift_num):
    rows, cols = (SY, SX)
    dark_pixel = dark_frame[bf_index].astype(jnp.float32) / 256.0
    gain_pixel = gain_frame[bf_index].astype(jnp.float32) / 4096.0
    corrected = (frames.astype(jnp.float32) - row_level[:, None, None] * dark_pixel) * gain_pixel
    ref_image = lax.optimization_barrier(jnp.sum(corrected, axis=2)).astype(jnp.bfloat16)
    pictures = jnp.transpose(corrected.astype(jnp.bfloat16), (2, 0, 1))
    del_rows = jnp.arange(rows, dtype=jnp.int32)
    col_range = jnp.arange(cols, dtype=jnp.int32)
    cosine_cols, sine_cols = phase_pair(col_range, col_range, cols)
    cosine_rows, sine_rows = phase_pair(del_rows, del_rows, rows)
    tables = tuple((t.astype(jnp.bfloat16) for t in (cosine_cols, sine_cols, cosine_rows, sine_rows)))
    up_rows_cos, up_rows_sin = phase_pair(jnp.arange(2 * rows, dtype=jnp.int32), signed_freq(rows), 2 * rows)
    up_rows_cos, up_rows_sin = (up_rows_cos.astype(jnp.bfloat16), up_rows_sin.astype(jnp.bfloat16))
    up_cols_cos, up_cols_sin = phase_pair(signed_freq(cols), jnp.arange(2 * cols, dtype=jnp.int32), 2 * cols)
    up_cols_cos, up_cols_sin = (up_cols_cos.astype(jnp.bfloat16), up_cols_sin.astype(jnp.bfloat16))
    lag_values = jnp.arange(LAGS, dtype=jnp.int32) - LAGS // 2
    lag_rows_cos, lag_rows_sin = phase_pair(lag_values, del_rows, rows)
    lag_rows_cos, lag_rows_sin = (lag_rows_cos.astype(jnp.bfloat16), lag_rows_sin.astype(jnp.bfloat16))
    lag_cols_cos, lag_cols_sin = phase_pair(col_range, lag_values, cols)
    lag_tables = (lag_rows_cos, lag_rows_sin, lag_cols_cos, lag_cols_sin)
    corr_scale = 1.0 / (rows * cols * math.sqrt(BF * rows * cols))
    ref_real, ref_imag = forward_pair(ref_image, *tables)

    def visit(totals, element):
        picture, amounts = element
        real_part, imag_part = forward_pair(picture, *tables)
        correl = correlate(real_part, imag_part, ref_real, ref_imag, lag_tables, corr_scale)
        real_shift, imag_shift = shift_apply(real_part, imag_part, amounts)
        total_real = totals[0] + matmul(up_rows_cos, real_shift) - matmul(up_rows_sin, imag_shift)
        total_imag = totals[1] + matmul(up_rows_cos, imag_shift) + matmul(up_rows_sin, real_shift)
        return ((total_real, total_imag), correl)
    start_totals = (jnp.zeros((2 * rows, cols), jnp.float32), jnp.zeros((2 * rows, cols), jnp.float32))
    totals, correls = lax.scan(visit, start_totals, (pictures, shift_num.T))
    rows_real = totals[0].astype(jnp.bfloat16)
    rows_imag = totals[1].astype(jnp.bfloat16)
    upsampled = (matmul(rows_real, up_cols_cos) - matmul(rows_imag, up_cols_sin)) * (1.0 / (rows * cols * math.sqrt(BF)))
    return (upsampled, correls)
```

```python
import functools
import math

import jax
import jax.numpy as jnp
import numpy as np
from jax import lax
from jax.experimental import pallas as pl
from jax.experimental.pallas import tpu as pltpu
from jax.sharding import PartitionSpec as P

LAGS = 16
DEN = 4
REACH = 32
PAD = REACH // DEN
AXES = ("scan", "grp")


def signed(length):
    k = np.arange(length)
    return np.where(k < length // 2, k, k - length)


def tables(product, period):
    angles = 2.0 * np.pi * (product % period) / period
    return jnp.asarray(np.cos(angles), jnp.bfloat16), jnp.asarray(np.sin(angles), jnp.bfloat16)


def low_dot(left, right, dims=((1,), (0,))):
    return lax.dot_general(left, right, (dims, ((), ())), preferred_element_type=jnp.float32)


def split_dot(table, values):
    upper = values.astype(jnp.bfloat16)
    lower = (values - upper.astype(jnp.float32)).astype(jnp.bfloat16)
    return low_dot(table, upper) + low_dot(table, lower)


def shift_add_kernel(shifts, v_ref, acc_ref):
    block, strip_rows, strip_cols = v_ref.shape
    tall, wide = acc_ref.shape[1:]
    step = pl.program_id(0)

    @pl.when(step == 0)
    def _():
        acc_ref[...] = jnp.zeros_like(acc_ref)

    def visit(j, carry):
        p = step * block + j
        sy = shifts[0, p] + REACH
        sx = shifts[1, p] + REACH
        kind = (sx & (DEN - 1)) * DEN + (sy & (DEN - 1))
        v = v_ref[j].astype(jnp.float32)
        v = jnp.concatenate([v, jnp.zeros((strip_rows, wide - strip_cols), jnp.float32)], axis=1)
        v = jnp.concatenate([v, jnp.zeros((tall - strip_rows, wide), jnp.float32)], axis=0)
        acc_ref[kind] += pltpu.roll(pltpu.roll(v, sy >> 2, 0), sx >> 2, 1)
        return carry

    lax.fori_loop(0, block, visit, 0, unroll=2)


def shift_add(shifts, images, tall, wide):
    pixels, strip_rows, strip_cols = images.shape
    block = math.gcd(pixels, 32)
    return pl.pallas_call(
        shift_add_kernel,
        out_shape=jax.ShapeDtypeStruct((DEN * DEN, tall, wide), jnp.float32),
        grid_spec=pltpu.PrefetchScalarGridSpec(
            num_scalar_prefetch=1,
            grid=(pixels // block,),
            in_specs=[pl.BlockSpec((block, strip_rows, strip_cols), lambda i, s: (i, 0, 0))],
            out_specs=pl.BlockSpec((DEN * DEN, tall, wide), lambda i, s: (0, 0, 0)),
        ),
        cost_estimate=pl.CostEstimate(flops=pixels * tall * wide * 8, bytes_accessed=images.size * 2, transcendentals=0),
        name="shift_add",
    )(shifts, images)


def local(frames, dark_frame, gain_frame, bf_index, row_level, shift_num):
    scan_count = lax.axis_size("scan")
    grp_count = lax.axis_size("grp")
    devices = scan_count * grp_count
    strip_rows, strip_cols, pixels = frames.shape
    rows, cols = strip_rows * scan_count, strip_cols * grp_count
    y0 = lax.axis_index("scan") * strip_rows
    x0 = lax.axis_index("grp") * strip_cols
    tall = strip_rows + 2 * PAD
    wide = -(-(strip_cols + 2 * PAD) // 128) * 128
    own_cols = cols // devices

    shifts = lax.all_gather(shift_num, AXES, axis=1, tiled=True)
    dark_pixel = jnp.take(dark_frame, bf_index).astype(jnp.float32) / 256.0
    gain_pixel = jnp.take(gain_frame, bf_index).astype(jnp.float32) / 4096.0
    corrected = (frames.astype(jnp.float32) - row_level[:, None, None] * dark_pixel) * gain_pixel
    ref_local = jnp.sum(corrected, axis=2).astype(jnp.bfloat16)
    strips = corrected.astype(jnp.bfloat16)
    ref_strip = lax.all_gather(ref_local, "grp", axis=1, tiled=True)
    ref_image = lax.all_gather(ref_strip, "scan", axis=0, tiled=True).astype(jnp.float32)

    sums = shift_add(shifts, jnp.transpose(strips, (2, 0, 1)), tall, wide)
    low_sums = sums.astype(jnp.bfloat16).reshape(DEN * DEN * tall, wide)
    kx = np.arange(cols)
    cols_cos, cols_sin = tables(kx[:, None] * np.arange(wide)[None, :], cols)
    zc = low_dot(cols_cos, low_sums, ((1,), (1,))).reshape(cols, DEN, DEN * tall)
    zs = low_dot(cols_sin, low_sums, ((1,), (1,))).reshape(cols, DEN, DEN * tall)
    turn = jnp.mod(
        DEN * jnp.asarray(kx, jnp.int32)[:, None] * (x0 - PAD)
        + jnp.asarray(signed(cols)[:, None] * np.arange(DEN)[None, :], jnp.int32),
        DEN * cols,
    ).astype(jnp.float32) * (2.0 * math.pi / (DEN * cols))
    turn_cos, turn_sin = jnp.cos(turn)[:, :, None], jnp.sin(turn)[:, :, None]
    part_real = jnp.sum(zc * turn_cos - zs * turn_sin, axis=1)
    part_imag = -jnp.sum(zc * turn_sin + zs * turn_cos, axis=1)
    part = jnp.concatenate([part_real, part_imag], axis=1).astype(jnp.bfloat16)

    part = lax.all_to_all(part, AXES, split_axis=0, concat_axis=0, tiled=True)
    part = part.reshape(scan_count, grp_count, own_cols, 2, DEN * tall).astype(jnp.float32)
    part = jnp.sum(part, axis=1).transpose(2, 1, 0, 3).reshape(2, own_cols, scan_count * DEN * tall)
    low_part = part.astype(jnp.bfloat16)
    ky = np.arange(rows)[:, None, None, None]
    place = (
        np.arange(scan_count)[:, None, None] * strip_rows + np.arange(tall)[None, None, :] - PAD
    )[None]
    turn_rows = DEN * ky * place + signed(rows)[:, None, None, None] * np.arange(DEN)[None, None, :, None]
    rows_cos, rows_sin = tables(turn_rows.reshape(rows, scan_count * DEN * tall), DEN * rows)
    last = ((1,), (1,))
    spec_real = low_dot(rows_cos, low_part[0], last) + low_dot(rows_sin, low_part[1], last)
    spec_imag = low_dot(rows_cos, low_part[1], last) - low_dot(rows_sin, low_part[0], last)
    device = lax.axis_index("scan") * grp_count + lax.axis_index("grp")
    anchor = (jnp.arange(rows)[:, None] == 0) & (jnp.arange(own_cols)[None, :] + device * own_cols == 0)
    spec = jnp.concatenate(
        [jnp.where(anchor, 0.0, spec_real), jnp.where(anchor, 0.0, spec_imag)], axis=1
    )
    up_rows_cos, up_rows_sin = tables(np.arange(2 * rows)[:, None] * signed(rows)[None, :], 2 * rows)
    by_cos, by_sin = split_dot(up_rows_cos, spec), split_dot(up_rows_sin, spec)
    column = jnp.concatenate(
        [
            by_cos[:, :own_cols] - by_sin[:, own_cols:],
            by_cos[:, own_cols:] + by_sin[:, :own_cols],
        ],
        axis=1,
    ).astype(jnp.bfloat16)
    column = lax.all_to_all(column, AXES, split_axis=0, concat_axis=0, tiled=True)
    own_rows = 2 * rows // devices
    column = column.reshape(devices, own_rows, 2, own_cols).transpose(2, 1, 0, 3).reshape(2, own_rows, cols)
    up_cols_cos, up_cols_sin = tables(signed(cols)[:, None] * np.arange(2 * cols)[None, :], 2 * cols)
    upsampled = (low_dot(column[0], up_cols_cos) - low_dot(column[1], up_cols_sin)) * (
        1.0 / (rows * cols * math.sqrt(pixels))
    )

    centred = (ref_image - jnp.mean(ref_image)).astype(jnp.bfloat16)
    half = LAGS // 2
    centred = jnp.concatenate([centred[-half:], centred, centred[:half]], axis=0)
    centred = jnp.concatenate([centred[:, -half:], centred, centred[:, :half]], axis=1)
    window = lax.dynamic_slice(centred, (y0, x0), (strip_rows + LAGS, strip_cols + LAGS))
    moved = jnp.stack([window[:, LAGS - b : LAGS - b + strip_cols] for b in range(LAGS)])
    moved = jnp.stack([moved[:, LAGS - a : LAGS - a + strip_rows] for a in range(LAGS)])
    moved = moved.reshape(LAGS * LAGS, strip_rows * strip_cols)
    correl = low_dot(strips.reshape(strip_rows * strip_cols, pixels), moved, ((0,), (1,)))
    correl = (correl * (1.0 / math.sqrt(pixels * rows * cols))).astype(jnp.bfloat16)
    correl = lax.all_to_all(correl, AXES, split_axis=0, concat_axis=0, tiled=True)
    correl = jnp.sum(correl.reshape(devices, pixels // devices, LAGS * LAGS).astype(jnp.float32), axis=0)
    return (upsampled, correl)


def solution(mesh):
    return jax.shard_map(
        local,
        mesh=mesh,
        in_specs=(P("scan", "grp", None), P(), P(), P(), P("scan"), P(None, ("scan", "grp"))),
        out_specs=(P(("scan", "grp"), None), P(("scan", "grp"), None)),
        check_vma=False,
    )
```
